32 devices in a mesh: gx: 4 (over y, x), gy: 2 (over core), gz: 4 (over z).
Axes of the slice: x: 2, y: 2, z: 4, core: 2. Of those that a mesh axis runs over, the one named last changes fastest.
Arguments:
- positions: float32 [3, 4, 2, 4, 128], P(None, 'gx', 'gy', 'gz'), may hold values from 0 to 22
- elements: int32 [4, 2, 4, 128], P('gx', 'gy', 'gz'), may hold values from 0 to 3
- prior_charges: float32 [4, 2, 4, 128], P('gx', 'gy', 'gz'), may hold values from -1.8 to 1.8
- neighbours: int32 [4, 2, 4, 128, 128], P('gx', 'gy', 'gz'), may hold values from 0 to 959, all different within a row; in each aligned block of 128 rows (0 to 127, 128 to 255, ..., all dimensions but the last counted through in order) at most 19 rows name the same one
- counts: int32 [4, 2, 4, 128], P('gx', 'gy', 'gz'), may hold values from 64 to 128
- boundary: int32 [4, 2, 4, 32], P('gx', 'gy', 'gz'), may hold values from 0 to 127, as said below
- wave_numbers: int32 [3, 2048], replicated, may hold values from -6 to 6, as said below
- hardness: float32 [4], replicated, may hold values from 3 to 9
- chi_first: bfloat16 [4, 32, 128], replicated, may hold values from -0.5 to 0.5
- chi_bias: float32 [4, 32], replicated, may hold values from -3 to 3
- chi_mid: bfloat16 [32, 4, 32], replicated, may hold values from -1 to 1
- chi_out: float32 [4, 32], replicated, may hold values from -1 to 1
- chi_offset: float32 [4], replicated, may hold values from -3 to 3
- short_first: bfloat16 [4, 32, 256], replicated, may hold values from -0.375 to 0.375
- short_charge: float32 [4, 32], replicated, may hold values from -4 to 4
- short_bias: float32 [4, 32], replicated, may hold values from -3 to 3
- short_mid: bfloat16 [32, 4, 32], replicated, may hold values from -1 to 1
- short_out: float32 [4, 32], replicated, may hold values from -1 to 1
- short_offset: float32 [4], replicated, may hold values from -3 to 3
Outputs:
- charges: float32 [4, 2, 4, 128], P('gx', 'gy', 'gz')
- energies: float32 [4, 2, 4, 128], P('gx', 'gy', 'gz')
The draws below stay inside these ranges and needn't reach their ends.
Inputs may be any that keep to these rules, and one draw needn't show every extreme that they name: `neighbours`: each row names 128 different indices; within one domain no index is named by more than 19 rows, a bound that some block reaches. `boundary`: the 32 indices of a domain are different. `wave_numbers`: every entry is nonzero.
All inputs are finite; a program needn't handle non-finite values.
Results may differ from the reference program's by a relative error of at most 0.0014.
Values sent between devices are 32-bit elements; how exact they have to be, the bound alone decides.
A program may use at most 64 MiB of HBM per device.

```python
import math
import jax
import jax.numpy as jnp
import numpy as np
from jax import lax

ATOMS_DEV = 128
GHOST = 32
NBR = 128
NB_MOST = 19
ELEM = 4
NBASIS = 32
FEAT = 128
HID = 32
KVEC = 2048
ITERS = 3
NGX = 4
NGY = 2
NGZ = 4


def draw_boundary(key, part):
    base = jax.random.fold_in(key, 17)
    keys = jax.random.split(base, NGX * NGY * NGZ)
    orders = jax.vmap(lambda single: jax.random.permutation(single, ATOMS_DEV))(keys)
    return orders[:, :GHOST].reshape(NGX, NGY, NGZ, GHOST).astype(jnp.int32)


def draw_wave_numbers(key, part):
    base = jax.random.fold_in(key, 29)
    size_key, sign_key = jax.random.split(base)
    magnitude = jax.random.randint(size_key, (3, KVEC), 1, 7)
    signs = jax.random.randint(sign_key, (3, KVEC), 0, 2) * 2 - 1
    return (magnitude * signs).astype(jnp.int32)


def with_ends(entries, rng, low, high):
    longest = entries.shape.index(max(entries.shape))
    spots = []
    for shift in (0, 1):
        where = [jax.random.randint(jax.random.fold_in(rng, axis), (), 0, length) for axis, length in enumerate(entries.shape)]
        where[longest] = (where[longest] + shift) % entries.shape[longest]
        spots.append(tuple(where))
    return entries.at[spots[0]].set(low).at[spots[1]].set(high)


def level_of(rng, extent, pieces, smallest, largest):
    loudness, own = 1.0, jax.random.fold_in(rng, 6)
    for axis_at, blocks in pieces:
        heights = jnp.exp(jax.random.uniform(jax.random.fold_in(own, axis_at), (blocks,), jnp.float32, smallest / len(pieces), largest / len(pieces)))
        loudness = loudness * jnp.repeat(heights, extent[axis_at] // blocks).reshape([-1 if axis == axis_at else 1 for axis in range(len(extent))])
    return loudness


def routed_block(stream_key, own, number, rows, number_of, top, reach, slope):
    ranking = jax.random.permutation(stream_key, number_of)
    crowded, usual = portions_of(number_of, rows * top, reach, slope, True), portions_of(number_of, rows * top, reach, slope, False)
    places = jnp.arange(number_of)

    def named(lengths, rotation):
        used = int((lengths > 0).sum())
        fixed = max(1, used // 4)
        moved = fixed + (places - fixed + rotation * (used - fixed)) % max(1, number_of - fixed)
        return jnp.zeros((number_of,), jnp.int32).at[ranking[jnp.where(places < fixed, places, moved)]].set(jnp.asarray(lengths, jnp.int32))

    lengths = jnp.where(number % 4 == 0, named(crowded, number // 4), named(usual, number - number // 4 - 1))
    mixed = jax.random.permutation(jax.random.fold_in(own, 3), number_of)
    donor, sink = mixed[0:number_of // 2 * 2:2], mixed[1:number_of // 2 * 2:2]
    slack = jnp.minimum(lengths[donor] - 1, reach - lengths[sink]) // 2
    slack = jnp.where((donor == ranking[0]) | (sink == ranking[0]) | (lengths[sink] == 0), 0, jnp.maximum(slack, 0))
    moved = jax.random.randint(jax.random.fold_in(own, 4), (number_of // 2,), 0, 1 << 20) % (slack + 1)
    lengths = lengths.at[donor].add(-moved).at[sink].add(moved)
    members = jnp.searchsorted(jnp.cumsum(lengths), jnp.arange(rows * top), side="right").astype(jnp.int32)
    table = members.reshape(top, rows).T
    table = table[jax.random.permutation(jax.random.fold_in(own, 1), rows)]
    rotation = jax.random.randint(jax.random.fold_in(own, 2), (rows, 1), 0, top)
    return jnp.take_along_axis(table, (jnp.arange(top)[None, :] + rotation) % top, axis=1)


def portions_of(number_of, total, limit, skew, full):
    weights = [(1 << 20) // math.isqrt(rank ** skew) + 1 for rank in range(1, number_of + 1)]
    largest = limit if full else min(limit, max(-(-total // number_of), total * weights[0] // sum(weights)))
    least = 1 if total - largest >= number_of - 1 else 0
    given, surplus = [largest] + [least] * (number_of - 1), total - largest - least * (number_of - 1)
    while surplus > 0:
        movable = [i for i in range(1, number_of) if given[i] < largest] or [i for i in range(1, number_of) if given[i] < limit]
        pool, left = sum([weights[i] for i in movable]), surplus
        for i in movable:
            more = min(limit - given[i], max(1, left * weights[i] // pool), surplus)
            given[i] = given[i] + more
            surplus = surplus - more
    return np.array(given)


def centred(own_key, extent, deviation, reach, pieces=(), kind=jnp.bfloat16):
    values = deviation * jax.random.normal(own_key, extent, jnp.float32)
    if pieces:
        values = values * level_of(own_key, extent, pieces, -0.22, 0.18)
    return jnp.clip(values, -reach, reach).astype(kind)


def setup_inputs(seed: int = 0) -> dict:
    splits = jax.random.split(jax.random.key(seed), 20)
    positions = jnp.clip(22.0 * jax.random.uniform(splits[0], (3, NGX, NGY, NGZ, ATOMS_DEV), jnp.float32) ** level_of(splits[0], (3, NGX, NGY, NGZ, ATOMS_DEV), ((1, 4), (2, 2), (3, 4)), -0.2, 0.2), 0.0, 22.0)
    elements = with_ends(jax.random.randint(splits[1], (NGX, NGY, NGZ, ATOMS_DEV), 0, ELEM), jax.random.fold_in(splits[1], 1), 0, ELEM - 1).astype(jnp.int32)
    prior_charges = centred(splits[2], (NGX, NGY, NGZ, ATOMS_DEV), 0.3, 1.8, ((0, 4), (1, 2), (2, 4)), jnp.float32)
    neighbours_keys = jax.random.split(jax.random.fold_in(splits[3], 1), NGX * NGY * NGZ * ATOMS_DEV // ATOMS_DEV)
    neighbours_turns = jax.random.permutation(jax.random.fold_in(splits[3], 3), NGX * NGY * NGZ * ATOMS_DEV // ATOMS_DEV)
    neighbours = jax.vmap(lambda own, number: routed_block(jax.random.fold_in(splits[3], 2), own, number, ATOMS_DEV, ATOMS_DEV + 26 * GHOST, NBR, NB_MOST, 0))(neighbours_keys, neighbours_turns).reshape((NGX, NGY, NGZ, ATOMS_DEV, NBR))
    counts = with_ends(jax.random.randint(splits[4], (NGX, NGY, NGZ, ATOMS_DEV), NBR // 2, NBR + 1), jax.random.fold_in(splits[4], 1), NBR // 2, NBR).astype(jnp.int32)
    boundary = draw_boundary(jax.random.fold_in(splits[19], 71), 0)
    wave_numbers = draw_wave_numbers(jax.random.fold_in(splits[19], 71), 0)
    hardness = jnp.clip(jnp.exp(jax.random.uniform(splits[7], (ELEM,), jnp.float32, math.log(3.0), math.log(9.0))), 3.0, 9.0)
    chi_first = centred(splits[8], (ELEM, HID, FEAT), FEAT ** -0.5, 0.5)
    chi_bias = centred(splits[9], (ELEM, HID), 0.5, 3.0, (), jnp.float32)
    chi_mid = centred(splits[10], (HID, ELEM, HID), HID ** -0.5, 1.0)
    chi_out = centred(splits[11], (ELEM, HID), HID ** -0.5, 1.0, (), jnp.float32)
    chi_offset = centred(splits[12], (ELEM,), 1.0, 3.0, (), jnp.float32)
    short_first = centred(splits[13], (ELEM, HID, 2 * FEAT), (2 * FEAT) ** -0.5, 0.375)
    short_charge = centred(splits[14], (ELEM, HID), 1.0, 4.0, (), jnp.float32)
    short_bias = centred(splits[15], (ELEM, HID), 0.5, 3.0, (), jnp.float32)
    short_mid = centred(splits[16], (HID, ELEM, HID), HID ** -0.5, 1.0)
    short_out = centred(splits[17], (ELEM, HID), HID ** -0.5, 1.0, (), jnp.float32)
    short_offset = centred(splits[18], (ELEM,), 1.0, 3.0, (), jnp.float32)
    return {"positions": positions, "elements": elements, "prior_charges": prior_charges, "neighbours": neighbours, "counts": counts, "boundary": boundary, "wave_numbers": wave_numbers, "hardness": hardness, "chi_first": chi_first, "chi_bias": chi_bias, "chi_mid": chi_mid, "chi_out": chi_out, "chi_offset": chi_offset, "short_first": short_first, "short_charge": short_charge, "short_bias": short_bias, "short_mid": short_mid, "short_out": short_out, "short_offset": short_offset}


DOMAIN = 22.0
SOFTENING = 22.0
SCREENING = 0.005
CUTOFF = 66.0
DAMPING = 0.1
COUPLING = 64.0
FEATURE_SCALE = 0.5
PAIR_STRENGTH = 1.0

def neighbour_offsets():
    table = []
    for first in range(3):
        for second in range(3):
            for third in range(3):
                if first * 9 + second * 3 + third != 13:
                    table.append((first - 1, second - 1, third - 1))
    return table

def pair_terms(own_place, gathered, slot_counts):
    slots = gathered.shape[2]
    separation = gathered[:3] - own_place[:, :, None]
    distance = jnp.sqrt(lax.optimization_barrier(jnp.sum(separation * separation, axis=0)))
    valid = (jnp.arange(slots, dtype=jnp.int32)[None, :] < slot_counts[:, None]).astype(jnp.float32)
    soft = jnp.sqrt(distance * distance + SOFTENING * SOFTENING)
    kernel = valid * (PAIR_STRENGTH / slots) * SOFTENING * lax.erfc(SCREENING * soft) / soft
    spacing = CUTOFF / (NBASIS - 1)
    centres = spacing * jnp.arange(NBASIS, dtype=jnp.float32)
    taper = valid * 0.5 * (1.0 + jnp.cos(jnp.pi * jnp.minimum(distance, CUTOFF) / CUTOFF))
    basis = jnp.exp(-0.5 * ((distance[None] - centres[:, None, None]) / spacing) ** 2) * taper[None]
    return (kernel, basis)

def element_network(features, kinds, weight_first, bias, weight_mid, weight_out, offset, extra):
    count, hidden, width = weight_first.shape
    activation = jnp.dot(weight_first.reshape(count * hidden, width), features, preferred_element_type=jnp.float32)
    activation = activation + bias.reshape(count * hidden, 1) + extra
    mask = jnp.repeat(kinds, hidden, axis=0)
    first = (jnp.tanh(activation) * mask).astype(jnp.bfloat16)
    second = jnp.tanh(jnp.dot(weight_mid.reshape(hidden, count * hidden), first, preferred_element_type=jnp.float32))
    chosen = lax.optimization_barrier(jnp.sum(weight_out[:, :, None] * kinds[:, None, :], axis=0))
    return lax.optimization_barrier(jnp.sum(second * chosen, axis=0)) + lax.optimization_barrier(jnp.sum(offset[:, None] * kinds, axis=0))

def phase_tile(waves, placed):
    theta = waves[0][:, None] * placed[0][None, :] + waves[1][:, None] * placed[1][None, :] + waves[2][:, None] * placed[2][None, :]
    return jnp.concatenate([jnp.cos(theta), jnp.sin(theta)], axis=0)

def ghosts(rows, boundary, move):
    picked = jnp.take_along_axis(rows, jnp.broadcast_to(boundary[None], (rows.shape[0],) + boundary.shape), axis=4)
    blocks = []
    for shift in neighbour_offsets():
        part = jnp.roll(picked, (-shift[0], -shift[1], -shift[2]), axis=(1, 2, 3))
        if move:
            moved = DOMAIN * jnp.array(shift, dtype=jnp.float32).reshape(3, 1, 1, 1, 1)
            part = jnp.concatenate([part[:3] + moved, part[3:]], axis=0)
        blocks.append(part)
    return jnp.concatenate(blocks, axis=4)

def reference(positions, elements, prior_charges, neighbours, counts, boundary, wave_numbers, hardness, chi_first, chi_bias, chi_mid, chi_out, chi_offset, short_first, short_charge, short_bias, short_mid, short_out, short_offset):
    domains = NGX * NGY * NGZ
    atoms = ATOMS_DEV
    highest = lax.Precision.HIGHEST
    kinds = (elements[None] == jnp.arange(ELEM, dtype=jnp.int32).reshape(ELEM, 1, 1, 1, 1)).astype(jnp.float32)
    rows = jnp.concatenate([positions, kinds, prior_charges[None]], axis=0)
    width = rows.shape[0]
    extended = jnp.concatenate([rows, ghosts(rows, boundary, True)], axis=4).reshape(width, domains, -1).transpose(1, 0, 2)
    own_places = positions.reshape(3, domains, atoms).transpose(1, 0, 2)
    lists = neighbours.reshape(domains, atoms, NBR)
    slot_counts = counts.reshape(domains, atoms)

    def geometry(inputs):
        own_place, ext_rows, near, count = inputs
        gathered = ext_rows[:, near]
        kernel, basis = pair_terms(own_place, gathered, count)
        descriptor = jnp.einsum('mis,eis->emi', basis, gathered[3:3 + ELEM], precision=highest)
        return (kernel, descriptor.reshape(FEAT, atoms))
    kernel, descriptor = lax.map(geometry, (own_places, extended, lists, slot_counts))
    descriptor_all = descriptor.transpose(1, 0, 2).reshape(FEAT, domains * atoms)
    onehot = kinds.reshape(ELEM, domains * atoms)
    features = (FEATURE_SCALE * descriptor_all).astype(jnp.bfloat16)
    negativity = element_network(features, onehot, chi_first, chi_bias, chi_mid, chi_out, chi_offset, 0.0).reshape(domains, atoms)
    stiffness = lax.optimization_barrier(jnp.sum(hardness[:, None] * onehot, axis=0)).reshape(domains, atoms)
    grid = jnp.stack(jnp.meshgrid(jnp.arange(NGX), jnp.arange(NGY), jnp.arange(NGZ), indexing='ij')).astype(jnp.float32)
    placed = (positions + DOMAIN * grid[..., None]).reshape(3, domains, atoms).transpose(1, 0, 2)
    box = DOMAIN * jnp.array([NGX, NGY, NGZ], dtype=jnp.float32)
    waves = 2.0 * jnp.pi * wave_numbers.astype(jnp.float32) / box[:, None]
    squared = lax.optimization_barrier(jnp.sum(waves * waves, axis=0))
    wave_weights = COUPLING * DAMPING ** 2 * jnp.exp(-squared / (4.0 * DAMPING ** 2)) / (squared * (domains * atoms))
    wave_weights = jnp.concatenate([wave_weights, wave_weights])

    def structure(vector):

        def add_domain(total, item):
            return (total + jnp.dot(phase_tile(waves, item[0]), item[1], precision=highest), None)
        total, ignored = lax.scan(add_domain, jnp.zeros((2 * KVEC,), jnp.float32), (placed, vector))
        return total

    def spread(weighted):
        return lax.map(lambda place: jnp.dot(weighted, phase_tile(waves, place), precision=highest), placed)

    def apply(vector):
        ghost_values = ghosts(vector.reshape(1, NGX, NGY, NGZ, atoms), boundary, False).reshape(domains, -1)
        ext_values = jnp.concatenate([vector, ghost_values], axis=1)
        near_values = jax.vmap(lambda values, near: values[near])(ext_values, lists)
        return stiffness * vector + lax.optimization_barrier(jnp.sum(kernel * near_values, axis=2)) + spread(wave_weights * structure(vector))
    charges = prior_charges.reshape(domains, atoms)
    residual = -negativity - apply(charges)
    direction = residual
    norm_now = jnp.sum(residual * residual)
    for step in range(ITERS):
        image = apply(direction)
        alpha = norm_now / jnp.sum(direction * image)
        charges = charges + alpha * direction
        residual = residual - alpha * image
        norm_next = jnp.sum(residual * residual)
        direction = residual + norm_next / norm_now * direction
        norm_now = norm_next
    ghost_charge = ghosts(charges.reshape(1, NGX, NGY, NGZ, atoms), boundary, False).reshape(domains, -1)
    extended_charge = jnp.concatenate([charges, ghost_charge], axis=1)

    def charge_geometry(inputs):
        own_place, ext_rows, near, count, values = inputs
        gathered = ext_rows[:, near]
        ignored, basis = pair_terms(own_place, gathered, count)
        weighted_kinds = gathered[3:3 + ELEM] * values[near][None]
        return jnp.einsum('mis,eis->emi', basis, weighted_kinds, precision=highest).reshape(FEAT, atoms)
    charge_descriptor = lax.map(charge_geometry, (own_places, extended, lists, slot_counts, extended_charge))
    charge_all = charge_descriptor.transpose(1, 0, 2).reshape(FEAT, domains * atoms)
    inputs_short = (FEATURE_SCALE * jnp.concatenate([descriptor_all, charge_all], axis=0)).astype(jnp.bfloat16)
    flat_charges = charges.reshape(domains * atoms)
    energies = element_network(inputs_short, onehot, short_first, short_bias, short_mid, short_out, short_offset, short_charge.reshape(-1, 1) * flat_charges[None, :])
    return (charges.reshape(NGX, NGY, NGZ, atoms), energies.reshape(NGX, NGY, NGZ, atoms))
```

```python
import functools
import math

import jax
import jax.numpy as jnp
import numpy as np
from jax import lax
from jax.experimental import pallas as pl
from jax.experimental.pallas import tpu as pltpu
from jax.sharding import PartitionSpec as P

NBASIS = 32
ITERS = 3
DOMAIN = 22.0
SOFTENING = 22.0
SCREENING = 0.005
CUTOFF = 66.0
DAMPING = 0.1
COUPLING = 64.0
FEATURE_SCALE = 0.5
PAIR_STRENGTH = 1.0
TOP = 6
LANES = 128
BINS = TOP * (2 * TOP) ** 2
CHUNKS = -(-BINS // LANES)
MESH = pl.DeviceIdType.MESH
AXES = ("gx", "gy", "gz")

OFFSETS = [
    (a, b, c) for a in (-1, 0, 1) for b in (-1, 0, 1) for c in (-1, 0, 1) if (a, b, c) != (0, 0, 0)
]


def wave_table(sizes, total_atoms):
    table = np.zeros((CHUNKS * LANES, 8), np.float64)
    signed = [n for n in range(-TOP, TOP + 1) if n != 0]
    spot = 0
    for nx in range(1, TOP + 1):
        for ny in signed:
            for nz in signed:
                k = 2.0 * np.pi * np.array([nx, ny, nz]) / (DOMAIN * np.array(sizes))
                squared = float((k * k).sum())
                weight = (
                    COUPLING * DAMPING**2 * math.exp(-squared / (4.0 * DAMPING**2)) / (squared * total_atoms)
                )
                table[spot, :4] = (nx, ny, nz, weight)
                spot += 1
    return table.reshape(CHUNKS, LANES, 8).transpose(0, 2, 1).astype(np.float32)


SIN_TERMS = [(-1) ** n * (2 * math.pi) ** (2 * n + 1) / math.factorial(2 * n + 1) for n in range(9)]
COS_TERMS = [(-1) ** n * (2 * math.pi) ** (2 * n) / math.factorial(2 * n) for n in range(10)]
ERF_TERMS = [
    2.0 / math.sqrt(math.pi) * (-1) ** n / (math.factorial(n) * (2 * n + 1)) for n in range(9)
]


def series(square, terms):
    total = jnp.full_like(square, terms[-1])
    for term in terms[-2::-1]:
        total = total * square + term
    return total


def unique_shifts(shifts, sizes):
    seen = []
    for shift in shifts:
        wrapped = tuple(s % n for s, n in zip(shift, sizes))
        if wrapped != (0, 0, 0) and wrapped not in seen:
            seen.append(wrapped)
    return seen


def negated(shift, sizes):
    return tuple((-s) % n for s, n in zip(shift, sizes))


def plan(sizes):
    halo = unique_shifts(OFFSETS, sizes)
    plane = unique_shifts([(a, b, 0) for a in range(sizes[0]) for b in range(sizes[1])], sizes)
    line = unique_shifts([(0, 0, c) for c in range(sizes[2])], sizes)
    return halo, plane, line


def kernel(
    sizes,
    hardness,
    chi_offset,
    short_offset,
    positions,
    elements,
    prior,
    neighbours,
    counts,
    picks,
    waves,
    table,
    columns,
    chi_first,
    chi_mid,
    short_first,
    short_mid,
    charges_out,
    energies_out,
    tile_cos,
    tile_sin,
    low_ref,
    high_ref,
    pair_ref,
    reach_ref,
    taper_ref,
    weights_ref,
    basis_ref,
    descriptor,
    own_ref,
    wave_weights,
    extended,
    halo_tile_out,
    halo_tile_in,
    halo_row_out,
    halo_row_in,
    plane_out,
    plane_in,
    line_out,
    line_in,
    tile_sems,
    row_sems,
    plane_sems,
    line_sems,
):
    halo, plane, line = plan(sizes)
    place = [lax.axis_index(name) for name in AXES]

    def device(shift):
        return tuple(lax.rem(p + s, n) if s else p for p, s, n in zip(place, shift, sizes))

    barrier = pltpu.get_barrier_semaphore()
    partners = unique_shifts(halo + plane + line, sizes)
    for shift in partners:
        pl.semaphore_signal(barrier, inc=1, device_id=device(shift), device_id_type=MESH)

    square = (LANES, LANES)

    def send(shifts, source, landing, sems):
        for shift in shifts:
            pltpu.make_async_remote_copy(
                src_ref=source,
                dst_ref=landing.at[shifts.index(negated(shift, sizes))],
                send_sem=sems.at[0],
                recv_sem=sems.at[1],
                device_id=device(shift),
                device_id_type=MESH,
            ).start()

    def landed(landing, sems):
        pltpu.make_async_copy(landing, landing, sems.at[1]).wait()

    def departed(landing, sems):
        pltpu.make_async_copy(landing, landing, sems.at[0]).wait()

    def column(row):
        return jnp.broadcast_to(row, square).T

    def pick_lanes(source, index):
        return jnp.take_along_axis(source, index, axis=1, mode="promise_in_bounds")

    turns = [
        column(
            (positions[d : d + 1, :] + DOMAIN * place[d].astype(jnp.float32)) * (1.0 / (DOMAIN * sizes[d]))
        )
        for d in range(3)
    ]

    own_ref[...] = jnp.zeros((8, LANES), jnp.float32)
    own_ref[0:3, :] = positions[...]
    own_ref[3:4, :] = elements[...].astype(jnp.float32)
    own_ref[4:5, :] = prior[...]
    picks8 = jnp.broadcast_to(picks[...], (8, LANES))
    halo_tile_out[...] = pick_lanes(own_ref[...], picks8)

    def fill(c, carry):
        lanes = table[c]
        theta = turns[0] * lanes[0:1] + turns[1] * lanes[1:2] + turns[2] * lanes[2:3]
        theta = theta - jnp.round(theta)
        squared = theta * theta
        tile_cos[c] = series(squared, COS_TERMS)
        tile_sin[c] = theta * series(squared, SIN_TERMS)
        return carry

    lax.fori_loop(0, CHUNKS, fill, 0)

    def structure(row, target):
        values = column(row)
        target[...] = jnp.zeros((16, LANES), jnp.float32)
        for c in range(CHUNKS):
            target[c : c + 1, :] = jnp.sum(tile_cos[c] * values, axis=0, keepdims=True)
            target[8 + c : 9 + c, :] = jnp.sum(tile_sin[c] * values, axis=0, keepdims=True)

    def spread(weighted):
        total = jnp.zeros(square, jnp.float32)
        for c in range(CHUNKS):
            total = total + tile_cos[c] * weighted[c : c + 1] + tile_sin[c] * weighted[8 + c : 9 + c]
        return jnp.sum(total.T, axis=0, keepdims=True)

    def reduce_start(phase):
        send(plane, plane_out.at[phase], plane_in.at[phase], plane_sems.at[phase])

    def reduce_middle(phase):
        landed(plane_in.at[phase], plane_sems.at[phase])
        line_out[phase] = plane_out[phase] + jnp.sum(plane_in[phase], axis=0)
        send(line, line_out.at[phase], line_in.at[phase], line_sems.at[phase])

    def reduce_end(phase):
        landed(line_in.at[phase], line_sems.at[phase])
        return line_out[phase] + jnp.sum(line_in[phase], axis=0)

    structure(prior[...], plane_out.at[0])
    pl.semaphore_wait(barrier, len(partners))
    send(halo, halo_tile_out, halo_tile_in, tile_sems)
    reduce_start(0)

    nearby = neighbours[...].T
    low_ref[...] = nearby & (LANES - 1)
    high_ref[...] = nearby >> 7
    lane8 = lax.broadcasted_iota(jnp.int32, (8, LANES), 1)
    lane_row = lax.broadcasted_iota(jnp.int32, (1, LANES), 1)
    row8 = lax.broadcasted_iota(jnp.int32, (8, LANES), 0)
    deep = lax.broadcasted_iota(jnp.int32, square, 0)

    def tally(p, sums):
        at = pl.ds(pl.multiple_of(p * LANES, LANES), LANES)
        nx, ny, nz = (waves[d : d + 1, at] for d in range(3))
        flip = jnp.where(nx < 0, -1, 1)
        nx, ny, nz = nx * flip, ny * flip, nz * flip
        ny = ny + jnp.where(ny < 0, TOP, TOP - 1)
        nz = nz + jnp.where(nz < 0, TOP, TOP - 1)
        spots = column((((nx - 1) * (2 * TOP) + ny) * (2 * TOP) + nz).astype(jnp.float32))
        return tuple(
            total
            + jnp.sum(
                jnp.where(spots == (lane_row + c * LANES).astype(jnp.float32), 1.0, 0.0), axis=0, keepdims=True
            )
            for c, total in enumerate(sums)
        )

    zero_row = jnp.zeros((1, LANES), jnp.float32)
    many = lax.fori_loop(0, waves.shape[1] // LANES, tally, (zero_row,) * CHUNKS)
    wave_weights[...] = jnp.zeros((16, LANES), jnp.float32)
    for c in range(CHUNKS):
        weighted_row = many[c] * table[c, 3:4, :]
        wave_weights[c : c + 1, :] = weighted_row
        wave_weights[8 + c : 9 + c, :] = weighted_row

    kind_row = elements[...]
    kinds = [jnp.where(kind_row == e, 1.0, 0.0) for e in range(4)]
    kind_mask = jnp.where((deep >> 5) == kind_row, 1.0, 0.0)
    stiffness = sum(kinds[e] * hardness[e] for e in range(4))
    shift_by = 0.25 * (hardness[0] + hardness[1] + hardness[2] + hardness[3])

    reduce_middle(0)
    landed(halo_tile_in, tile_sems)

    slots = [halo.index(tuple(s % n for s, n in zip(o, sizes))) for o in OFFSETS]

    def merge(fetch, lanes, chunk):
        out = fetch(4 * chunk)
        for q in range(1, 4):
            if 4 * chunk + q < len(OFFSETS):
                out = jnp.where(lanes >= 32 * q, fetch(4 * chunk + q), out)
        return out

    def moved(block):
        o = OFFSETS[block]
        by = jnp.where(
            row8 == 0, DOMAIN * o[0], jnp.where(row8 == 1, DOMAIN * o[1], jnp.where(row8 == 2, DOMAIN * o[2], 0.0))
        )
        return halo_tile_in[slots[block]] + by

    tiles = [own_ref[...]] + [merge(moved, lane8, c) for c in range(7)]

    def gather(rows):
        low, high = low_ref[...], high_ref[...]
        out = jnp.zeros(square, jnp.float32)
        for c in range(8):
            out = jnp.where(high == c, pick_lanes(jnp.broadcast_to(rows[c], square), low), out)
        return out

    total = jnp.zeros(square, jnp.float32)
    for d in range(3):
        gap = gather([tile[d : d + 1] for tile in tiles]) - positions[d : d + 1, :]
        total = total + gap * gap
    distance = jnp.sqrt(total)
    valid = jnp.where(deep < counts[...], 1.0, 0.0)
    soft_square = total + SOFTENING * SOFTENING
    soft = jnp.sqrt(soft_square)
    far = SCREENING * soft
    erfc = 1.0 - far * series(far * far, ERF_TERMS)
    pair_ref[...] = valid * (PAIR_STRENGTH / LANES * SOFTENING) * erfc / soft
    half = jnp.minimum(distance, CUTOFF) * (0.5 / CUTOFF)
    taper_ref[...] = valid * 0.5 * (1.0 + series(half * half, COS_TERMS))
    reach_ref[...] = distance * ((NBASIS - 1) / CUTOFF)
    near_kind = gather([tile[3:4] for tile in tiles])
    for e in range(4):
        weights_ref[e] = jnp.where(near_kind == float(e), 1.0, 0.0)
    for c in range(8):
        extended[0, c : c + 1, :] = tiles[c][4:5]

    def describe(m, carry):
        away = reach_ref[...] - m.astype(jnp.float32)
        basis = jnp.exp(-0.5 * (away * away)) * taper_ref[...]
        basis_ref[m] = basis
        for e in range(4):
            descriptor[0, e, pl.ds(m, 1), :] = jnp.sum(basis * weights_ref[e], axis=0, keepdims=True)
        return carry

    lax.fori_loop(0, NBASIS, describe, 0)

    def network(inputs, first_weights, bias, mid, out_column, offset, extra):
        activation = jnp.dot(first_weights, inputs, preferred_element_type=jnp.float32) + bias
        if extra is not None:
            activation = activation + extra
        first = (jnp.tanh(activation) * kind_mask).astype(jnp.bfloat16)
        second = jnp.tanh(jnp.dot(mid, first, preferred_element_type=jnp.float32))
        chosen = sum(columns[32 * e : 32 * e + 32, out_column : out_column + 1] * kinds[e] for e in range(4))
        result = jnp.sum(second * chosen, axis=0, keepdims=True)
        return result + sum(kinds[e] * offset[e] for e in range(4))

    features = (FEATURE_SCALE * descriptor[0].reshape(LANES, LANES)).astype(jnp.bfloat16)
    negativity = network(features, chi_first[...], columns[:, 0:1], chi_mid[...], 3, chi_offset, None)

    def local(vector, phase):
        rows = [extended[phase, c : c + 1, :] for c in range(8)]
        return stiffness * vector + jnp.sum(pair_ref[...] * gather(rows), axis=0, keepdims=True)

    vectors = []
    vector = prior[...]
    near_part = local(vector, 0)
    vector = -negativity - (near_part + spread(wave_weights[...] * reduce_end(0)))
    vectors.append(vector)
    for step in range(ITERS):
        phase = step + 1
        picked = pick_lanes(jnp.broadcast_to(vector, (8, LANES)), picks8)
        halo_row_out[step] = picked[0:1]
        structure(vector, plane_out.at[phase])
        reduce_start(phase)
        send(halo, halo_row_out.at[step], halo_row_in.at[step], row_sems.at[step])
        reduce_middle(phase)
        landed(halo_row_in.at[step], row_sems.at[step])
        extended[phase, 0:1, :] = vector
        for c in range(7):
            extended[phase, c + 1 : c + 2, :] = merge(lambda b: halo_row_in[step, slots[b]], lane_row, c)
        near_part = local(vector, phase) - shift_by * vector
        vector = near_part + spread(wave_weights[...] * reduce_end(phase))
        vectors.append(vector)

    last = ITERS + 1
    pairs = [(a, b) for a in range(last) for b in range(a, last)]
    plane_out[last] = jnp.zeros((16, LANES), jnp.float32)
    for spot, (a, b) in enumerate(pairs):
        plane_out[last, spot : spot + 1, :] = vectors[a] * vectors[b]
    reduce_start(last)
    reduce_middle(last)
    inner = jnp.broadcast_to(jnp.sum(reduce_end(last), axis=1, keepdims=True), (16, LANES))
    gram = {}
    for spot, (a, b) in enumerate(pairs):
        gram[a, b] = gram[b, a] = inner[spot : spot + 1]

    def product(left, right):
        return sum(x * y * gram[a, b] for a, x in enumerate(left) for b, y in enumerate(right))

    one = jnp.ones((1, LANES), jnp.float32)
    residual, direction, solution_part = [one], [one], []
    norm = product(residual, residual)
    for step in range(ITERS):
        image = [shift_by * x for x in direction] + [jnp.zeros_like(one)]
        for a, x in enumerate(direction):
            image[a + 1] = image[a + 1] + x
        alpha = norm / product(direction, image)
        padded = solution_part + [jnp.zeros_like(one)] * (len(direction) - len(solution_part))
        solution_part = [s + alpha * x for s, x in zip(padded, direction)]
        if step + 1 < ITERS:
            longer = residual + [jnp.zeros_like(one)]
            residual = [r - alpha * i for r, i in zip(longer, image)]
            after = product(residual, residual)
            ratio = after / norm
            direction = [r + ratio * x for r, x in zip(residual, direction + [jnp.zeros_like(one)])]
            norm = after

    answer = extended[0]
    for a, x in enumerate(solution_part):
        answer = answer + x * extended[a + 1]
    charges = answer[0:1]
    charges_out[...] = charges

    near_charge = gather([answer[c : c + 1] for c in range(8)])
    for e in range(4):
        weights_ref[e] = weights_ref[e] * near_charge

    def describe_charge(m, carry):
        basis = basis_ref[m]
        for e in range(4):
            descriptor[1, e, pl.ds(m, 1), :] = jnp.sum(basis * weights_ref[e], axis=0, keepdims=True)
        return carry

    lax.fori_loop(0, NBASIS, describe_charge, 0)
    inputs = (FEATURE_SCALE * descriptor[...].reshape(2 * LANES, LANES)).astype(jnp.bfloat16)
    energies_out[...] = network(
        inputs, short_first[...], columns[:, 1:2], short_mid[...], 4, short_offset, columns[:, 2:3] * charges
    )

    departed(halo_tile_in, tile_sems)
    for step in range(ITERS):
        departed(halo_row_in.at[step], row_sems.at[step])
    for phase in range(ITERS + 2):
        departed(plane_in.at[phase], plane_sems.at[phase])
        departed(line_in.at[phase], line_sems.at[phase])


def body(
    sizes,
    positions,
    elements,
    prior_charges,
    neighbours,
    counts,
    boundary,
    wave_numbers,
    hardness,
    chi_first,
    chi_bias,
    chi_mid,
    chi_out,
    chi_offset,
    short_first,
    short_charge,
    short_bias,
    short_mid,
    short_out,
    short_offset,
):
    atoms = positions.shape[-1]
    halo, plane, line = plan(sizes)
    table = wave_table(sizes, atoms * sizes[0] * sizes[1] * sizes[2])
    columns = jnp.stack(
        [x.reshape(-1) for x in (chi_bias, short_bias, short_charge, chi_out, short_out)], axis=1
    )
    vmem = pl.BlockSpec(memory_space=pltpu.VMEM)
    smem = pl.BlockSpec(memory_space=pltpu.SMEM)
    f32 = jnp.float32
    phases = ITERS + 2
    row = jax.ShapeDtypeStruct((1, atoms), f32)
    charges, energies = pl.pallas_call(
        functools.partial(kernel, sizes),
        out_shape=(row, row),
        in_specs=[smem] * 3 + [vmem] * 13,
        out_specs=(vmem, vmem),
        scratch_shapes=[
            pltpu.VMEM((CHUNKS, LANES, LANES), f32),
            pltpu.VMEM((CHUNKS, LANES, LANES), f32),
            pltpu.VMEM((LANES, LANES), jnp.int32),
            pltpu.VMEM((LANES, LANES), jnp.int32),
            pltpu.VMEM((LANES, LANES), f32),
            pltpu.VMEM((LANES, LANES), f32),
            pltpu.VMEM((LANES, LANES), f32),
            pltpu.VMEM((4, LANES, LANES), f32),
            pltpu.VMEM((NBASIS, LANES, LANES), f32),
            pltpu.VMEM((2, 4, NBASIS, LANES), f32),
            pltpu.VMEM((8, LANES), f32),
            pltpu.VMEM((16, LANES), f32),
            pltpu.VMEM((ITERS + 1, 8, LANES), f32),
            pltpu.VMEM((8, LANES), f32),
            pltpu.VMEM((len(halo), 8, LANES), f32),
            pltpu.VMEM((ITERS, 1, LANES), f32),
            pltpu.VMEM((ITERS, len(halo), 1, LANES), f32),
            pltpu.VMEM((phases, 16, LANES), f32),
            pltpu.VMEM((phases, len(plane), 16, LANES), f32),
            pltpu.VMEM((phases, 16, LANES), f32),
            pltpu.VMEM((phases, len(line), 16, LANES), f32),
            pltpu.SemaphoreType.DMA((2,)),
            pltpu.SemaphoreType.DMA((ITERS, 2)),
            pltpu.SemaphoreType.DMA((phases, 2)),
            pltpu.SemaphoreType.DMA((phases, 2)),
        ],
        compiler_params=pltpu.CompilerParams(collective_id=0, has_side_effects=True),
    )(
        hardness,
        chi_offset,
        short_offset,
        positions.reshape(3, atoms),
        elements.reshape(1, atoms),
        prior_charges.reshape(1, atoms),
        neighbours.reshape(atoms, atoms),
        counts.reshape(1, atoms),
        jnp.tile(boundary.reshape(1, -1), (1, 4)),
        wave_numbers,
        jnp.asarray(table),
        columns,
        chi_first.reshape(atoms, -1),
        chi_mid.reshape(NBASIS, -1),
        short_first.reshape(atoms, -1),
        short_mid.reshape(NBASIS, -1),
    )
    return (charges.reshape(1, 1, 1, atoms), energies.reshape(1, 1, 1, atoms))


def solution(mesh):
    sizes = tuple(mesh.shape[name] for name in AXES)
    spread_over = P("gx", "gy", "gz", None)
    in_specs = (
        P(None, "gx", "gy", "gz", None),
        spread_over,
        spread_over,
        P("gx", "gy", "gz", None, None),
        spread_over,
        spread_over,
    ) + (P(),) * 13
    return jax.shard_map(
        functools.partial(body, sizes),
        mesh=mesh,
        in_specs=in_specs,
        out_specs=(spread_over, spread_over),
        check_vma=False,
    )
```

```python
import functools
import math

import jax
import jax.numpy as jnp
import numpy as np
from jax import lax
from jax.experimental import pallas as pl
from jax.experimental.pallas import tpu as pltpu
from jax.sharding import PartitionSpec as P

NBASIS = 32
ITERS = 3
DOMAIN = 22.0
SOFTENING = 22.0
SCREENING = 0.005
CUTOFF = 66.0
DAMPING = 0.1
COUPLING = 64.0
FEATURE_SCALE = 0.5
PAIR_STRENGTH = 1.0
TOP = 6
LANES = 128
BINS = TOP * (2 * TOP) ** 2
CHUNKS = -(-BINS // LANES)
MESH = pl.DeviceIdType.MESH
AXES = ("gx", "gy", "gz")

OFFSETS = [
    (a, b, c) for a in (-1, 0, 1) for b in (-1, 0, 1) for c in (-1, 0, 1) if (a, b, c) != (0, 0, 0)
]


def wave_table(sizes, total_atoms):
    table = np.zeros((CHUNKS * LANES, 8), np.float64)
    signed = [n for n in range(-TOP, TOP + 1) if n != 0]
    spot = 0
    for nx in range(1, TOP + 1):
        for ny in signed:
            for nz in signed:
                k = 2.0 * np.pi * np.array([nx, ny, nz]) / (DOMAIN * np.array(sizes))
                squared = float((k * k).sum())
                weight = (
                    COUPLING * DAMPING**2 * math.exp(-squared / (4.0 * DAMPING**2)) / (squared * total_atoms)
                )
                table[spot, :4] = (nx, ny, nz, weight)
                spot += 1
    return table.reshape(CHUNKS, LANES, 8).transpose(0, 2, 1).astype(np.float32)


SIN_TERMS = [(-1) ** n * (2 * math.pi) ** (2 * n + 1) / math.factorial(2 * n + 1) for n in range(9)]
COS_TERMS = [(-1) ** n * (2 * math.pi) ** (2 * n) / math.factorial(2 * n) for n in range(10)]
ERF_TERMS = [
    2.0 / math.sqrt(math.pi) * (-1) ** n / (math.factorial(n) * (2 * n + 1)) for n in range(9)
]


def series(square, terms):
    total = jnp.full_like(square, terms[-1])
    for term in terms[-2::-1]:
        total = total * square + term
    return total


def unique_shifts(shifts, sizes):
    seen = []
    for shift in shifts:
        wrapped = tuple(s % n for s, n in zip(shift, sizes))
        if wrapped != (0, 0, 0) and wrapped not in seen:
            seen.append(wrapped)
    return seen


def negated(shift, sizes):
    return tuple((-s) % n for s, n in zip(shift, sizes))


def plan(sizes):
    halo = unique_shifts(OFFSETS, sizes)
    plane = unique_shifts([(a, b, 0) for a in range(sizes[0]) for b in range(sizes[1])], sizes)
    line = unique_shifts([(0, 0, c) for c in range(sizes[2])], sizes)
    return halo, plane, line


def kernel(
    sizes,
    hardness,
    chi_offset,
    short_offset,
    positions,
    elements,
    prior,
    neighbours,
    counts,
    boundary,
    waves,
    table,
    chi_bias,
    short_bias,
    short_charge,
    chi_out,
    short_out,
    chi_first,
    chi_mid,
    short_first,
    short_mid,
    charges_out,
    energies_out,
    tile_cos,
    tile_sin,
    low_ref,
    high_ref,
    pair_ref,
    reach_ref,
    taper_ref,
    weights_ref,
    basis_ref,
    descriptor,
    own_ref,
    picks_ref,
    pack_ref,
    mid_ref,
    near_kind_ref,
    totals_ref,
    wave_weights,
    extended,
    halo_tile_out,
    halo_tile_in,
    halo_row_out,
    halo_row_in,
    plane_out,
    plane_in,
    line_out,
    line_in,
    dot_plane_out,
    dot_plane_in,
    dot_line_out,
    dot_line_in,
    tile_sems,
    row_sems,
    plane_sems,
    line_sems,
    dot_sems,
):
    halo, plane, line = plan(sizes)
    place = [lax.axis_index(name) for name in AXES]

    def device(shift):
        return tuple(lax.rem(p + s, n) if s else p for p, s, n in zip(place, shift, sizes))

    barrier = pltpu.get_barrier_semaphore()
    partners = unique_shifts(halo + plane + line, sizes)
    for shift in partners:
        pl.semaphore_signal(barrier, inc=1, device_id=device(shift), device_id_type=MESH)

    square = (LANES, LANES)

    def send(shifts, source, landing, sems):
        for shift in shifts:
            pltpu.make_async_remote_copy(
                src_ref=source,
                dst_ref=landing.at[shifts.index(negated(shift, sizes))],
                send_sem=sems.at[0],
                recv_sem=sems.at[1],
                device_id=device(shift),
                device_id_type=MESH,
            ).start()

    def landed(landing, sems):
        pltpu.make_async_copy(landing, landing, sems.at[1]).wait()

    def departed(landing, sems):
        pltpu.make_async_copy(landing, landing, sems.at[0]).wait()

    def column(row):
        return jnp.broadcast_to(row, square).T

    def pick_lanes(source, index):
        return jnp.take_along_axis(source, index, axis=1, mode="promise_in_bounds")

    turns = [
        column(
            (positions[d] + DOMAIN * place[d].astype(jnp.float32)) * (1.0 / (DOMAIN * sizes[d]))
        )
        for d in range(3)
    ]

    own_ref[...] = jnp.zeros((8, LANES), jnp.float32)
    for d in range(3):
        own_ref[d : d + 1, :] = positions[d]
    own_ref[3:4, :] = elements[...].astype(jnp.float32)
    own_ref[4:5, :] = prior[...]
    lane8 = lax.broadcasted_iota(jnp.int32, (8, LANES), 1)
    width = boundary.shape[1]
    picks_ref[...] = jnp.zeros((8, LANES), jnp.int32)
    picks_ref[0:1, 0:width] = boundary[...]
    picks8 = pick_lanes(jnp.broadcast_to(picks_ref[0:1, :], (8, LANES)), lane8 & (width - 1))
    halo_tile_out[...] = pick_lanes(own_ref[...], picks8)

    def fill(c, carry):
        lanes = table[c]
        theta = turns[0] * lanes[0:1] + turns[1] * lanes[1:2] + turns[2] * lanes[2:3]
        theta = theta - jnp.round(theta)
        squared = theta * theta
        tile_cos[c] = series(squared, COS_TERMS)
        tile_sin[c] = theta * series(squared, SIN_TERMS)
        return carry

    lax.fori_loop(0, CHUNKS, fill, 0)

    def structure(row, target):
        values = column(row)
        target[...] = jnp.zeros((16, LANES), jnp.float32)
        for c in range(CHUNKS):
            target[c : c + 1, :] = jnp.sum(tile_cos[c] * values, axis=0, keepdims=True)
            target[8 + c : 9 + c, :] = jnp.sum(tile_sin[c] * values, axis=0, keepdims=True)

    def spread(weighted):
        total = jnp.zeros(square, jnp.float32)
        for c in range(CHUNKS):
            total = total + tile_cos[c] * weighted[c : c + 1] + tile_sin[c] * weighted[8 + c : 9 + c]
        return jnp.sum(total.T, axis=0, keepdims=True)

    def reduce_start(phase):
        send(plane, plane_out.at[phase], plane_in.at[phase], plane_sems.at[phase])

    def reduce_middle(phase):
        landed(plane_in.at[phase], plane_sems.at[phase])
        line_out[phase] = plane_out[phase] + jnp.sum(plane_in[phase], axis=0)
        send(line, line_out.at[phase], line_in.at[phase], line_sems.at[phase])

    def reduce_end(phase):
        landed(line_in.at[phase], line_sems.at[phase])
        return line_out[phase] + jnp.sum(line_in[phase], axis=0)

    nearby = neighbours[...].T
    low_ref[...] = nearby & (LANES - 1)
    high_ref[...] = nearby >> 7
    lane_row = lax.broadcasted_iota(jnp.int32, (1, LANES), 1)
    row8 = lax.broadcasted_iota(jnp.int32, (8, LANES), 0)
    deep = lax.broadcasted_iota(jnp.int32, square, 0)

    def tally(p, sums):
        at = pl.ds(pl.multiple_of(p * LANES, LANES), LANES)
        nx, ny, nz = (waves[d : d + 1, at] for d in range(3))
        flip = jnp.where(nx < 0, -1, 1)
        nx, ny, nz = nx * flip, ny * flip, nz * flip
        ny = ny + jnp.where(ny < 0, TOP, TOP - 1)
        nz = nz + jnp.where(nz < 0, TOP, TOP - 1)
        spots = column((((nx - 1) * (2 * TOP) + ny) * (2 * TOP) + nz).astype(jnp.float32))
        return tuple(
            total
            + jnp.sum(
                jnp.where(spots == (lane_row + c * LANES).astype(jnp.float32), 1.0, 0.0), axis=0, keepdims=True
            )
            for c, total in enumerate(sums)
        )

    zero_row = jnp.zeros((1, LANES), jnp.float32)
    many = lax.fori_loop(0, waves.shape[1] // LANES, tally, (zero_row,) * CHUNKS)
    wave_weights[...] = jnp.zeros((16, LANES), jnp.float32)
    for c in range(CHUNKS):
        weighted_row = many[c] * table[c, 3:4, :]
        wave_weights[c : c + 1, :] = weighted_row
        wave_weights[8 + c : 9 + c, :] = weighted_row

    kind_row = elements[...]
    kinds = [jnp.where(kind_row == e, 1.0, 0.0) for e in range(4)]
    kind_mask = jnp.where((deep >> 5) == kind_row, 1.0, 0.0)
    stiffness = sum(kinds[e] * hardness[e] for e in range(4))
    shift_by = 0.25 * (hardness[0] + hardness[1] + hardness[2] + hardness[3])

    pack_ref[...] = jnp.zeros(square, jnp.float32)
    for spot, part in enumerate((chi_bias, short_bias, short_charge, chi_out, short_out)):
        pack_ref[4 * spot : 4 * spot + 4, 0:32] = part[...]
    pack_ref[...] = pack_ref[...].T

    def parameter(spot):
        return [pack_ref[0:32, 4 * spot + e : 4 * spot + e + 1] for e in range(4)]

    def stacked(spot):
        return jnp.concatenate([jnp.broadcast_to(x, (32, LANES)) for x in parameter(spot)], axis=0)

    for spot, mid in enumerate((chi_mid, short_mid)):
        wide = mid[...].astype(jnp.float32)
        for e in range(4):
            mid_ref[spot, :, 32 * e : 32 * e + 32] = wide[:, e, :]

    structure(prior[...], plane_out.at[0])
    pl.semaphore_wait(barrier, len(partners))
    send(halo, halo_tile_out, halo_tile_in, tile_sems)
    reduce_start(0)

    reduce_middle(0)
    landed(halo_tile_in, tile_sems)

    slots = [halo.index(tuple(s % n for s, n in zip(o, sizes))) for o in OFFSETS]

    def merge(fetch, lanes, chunk):
        out = fetch(4 * chunk)
        for q in range(1, 4):
            if 4 * chunk + q < len(OFFSETS):
                out = jnp.where(lanes >= 32 * q, fetch(4 * chunk + q), out)
        return out

    def moved(block):
        o = OFFSETS[block]
        by = jnp.where(
            row8 == 0, DOMAIN * o[0], jnp.where(row8 == 1, DOMAIN * o[1], jnp.where(row8 == 2, DOMAIN * o[2], 0.0))
        )
        return halo_tile_in[slots[block]] + by

    tiles = [own_ref[...]] + [merge(moved, lane8, c) for c in range(7)]

    def gather(rows):
        low, high = low_ref[...], high_ref[...]
        out = jnp.zeros(square, jnp.float32)
        for c in range(8):
            out = jnp.where(high == c, pick_lanes(jnp.broadcast_to(rows[c], square), low), out)
        return out

    total = jnp.zeros(square, jnp.float32)
    for d in range(3):
        gap = gather([tile[d : d + 1] for tile in tiles]) - positions[d]
        total = total + gap * gap
    distance = jnp.sqrt(total)
    valid = jnp.where(deep < counts[...], 1.0, 0.0)
    soft_square = total + SOFTENING * SOFTENING
    soft = jnp.sqrt(soft_square)
    far = SCREENING * soft
    erfc = 1.0 - far * series(far * far, ERF_TERMS)
    pair_ref[...] = valid * (PAIR_STRENGTH / LANES * SOFTENING) * erfc / soft
    half = jnp.minimum(distance, CUTOFF) * (0.5 / CUTOFF)
    taper_ref[...] = valid * 0.5 * (1.0 + series(half * half, COS_TERMS))
    reach_ref[...] = distance * ((NBASIS - 1) / CUTOFF)
    near_kind = gather([tile[3:4] for tile in tiles])
    near_kind_ref[...] = near_kind
    for e in range(4):
        weights_ref[e] = jnp.where(near_kind == float(e), 1.0, 0.0)
    for c in range(8):
        extended[0, c : c + 1, :] = tiles[c][4:5]

    def describe(m, carry):
        away = reach_ref[...] - m.astype(jnp.float32)
        basis = jnp.exp(-0.5 * (away * away)) * taper_ref[...]
        basis_ref[m] = basis
        for e in range(4):
            descriptor[0, e, pl.ds(m, 1), :] = jnp.sum(basis * weights_ref[e], axis=0, keepdims=True)
        return carry

    lax.fori_loop(0, NBASIS, describe, 0)

    def network(inputs, first_weights, bias, mid, out_spot, offset, extra):
        activation = jnp.dot(first_weights, inputs, preferred_element_type=jnp.float32) + bias
        if extra is not None:
            activation = activation + extra
        first = (jnp.tanh(activation) * kind_mask).astype(jnp.bfloat16)
        second = jnp.tanh(jnp.dot(mid.astype(jnp.bfloat16), first, preferred_element_type=jnp.float32))
        chosen = sum(x * kinds[e] for e, x in enumerate(parameter(out_spot)))
        result = jnp.sum(second * chosen, axis=0, keepdims=True)
        return result + sum(kinds[e] * offset[e] for e in range(4))

    features = (FEATURE_SCALE * descriptor[0].reshape(LANES, LANES)).astype(jnp.bfloat16)
    negativity = network(features, chi_first[...], stacked(0), mid_ref[0], 3, chi_offset, None)

    def local(vector, phase):
        near = gather([extended[phase, c : c + 1, :] for c in range(8)])
        return near, stiffness * vector + jnp.sum(pair_ref[...] * near, axis=0, keepdims=True)

    def describe_charges(near, phase):
        for e in range(4):
            weights_ref[e] = jnp.where(near_kind_ref[...] == float(e), near, 0.0)

        def part(m, carry):
            basis = basis_ref[m]
            for e in range(4):
                descriptor[1 + phase, e, pl.ds(m, 1), :] = jnp.sum(
                    basis * weights_ref[e], axis=0, keepdims=True
                )
            return carry

        lax.fori_loop(0, NBASIS, part, 0)

    near, near_part = local(prior[...], 0)
    vector = -negativity - (near_part + spread(wave_weights[...] * reduce_end(0)))
    vectors = [vector]
    for step in range(ITERS):
        phase = step + 1
        picked = pick_lanes(jnp.broadcast_to(vector, (8, LANES)), picks8)
        halo_row_out[step] = picked[0:1]
        structure(vector, plane_out.at[phase])
        reduce_start(phase)
        send(halo, halo_row_out.at[step], halo_row_in.at[step], row_sems.at[step])
        describe_charges(near, step)
        reduce_middle(phase)
        landed(halo_row_in.at[step], row_sems.at[step])
        extended[phase, 0:1, :] = vector
        for c in range(7):
            extended[phase, c + 1 : c + 2, :] = merge(lambda b: halo_row_in[step, slots[b]], lane_row, c)
        near, near_part = local(vector, phase)
        near_part = near_part - shift_by * vector
        if phase < ITERS:
            totals_ref[step] = reduce_end(phase)
            vector = near_part + spread(wave_weights[...] * totals_ref[step])
            vectors.append(vector)

    pairs = [(a, b) for a in range(ITERS) for b in range(a, ITERS)]
    rows = [vectors[a] * vectors[b] for a, b in pairs] + [x * near_part for x in vectors]
    pairs = pairs + [(a, ITERS) for a in range(ITERS)]
    dot_plane_out[...] = jnp.zeros((16, LANES), jnp.float32)
    for spot, row in enumerate(rows):
        dot_plane_out[spot : spot + 1, :] = row
    send(plane, dot_plane_out, dot_plane_in, dot_sems.at[0])
    totals_ref[ITERS - 1] = reduce_end(ITERS)
    landed(dot_plane_in, dot_sems.at[0])
    dot_line_out[...] = dot_plane_out[...] + jnp.sum(dot_plane_in[...], axis=0)
    send(line, dot_line_out, dot_line_in, dot_sems.at[1])
    describe_charges(near, ITERS)
    weighted = wave_weights[...] * totals_ref[ITERS - 1]
    energies = [
        jnp.sum(jnp.sum(weighted * totals_ref[a], axis=0, keepdims=True), axis=1, keepdims=True)
        for a in range(ITERS)
    ]
    landed(dot_line_in, dot_sems.at[1])
    inner = dot_line_out[...] + jnp.sum(dot_line_in[...], axis=0)
    inner = jnp.broadcast_to(jnp.sum(inner, axis=1, keepdims=True), (16, LANES))
    gram = {}
    for spot, (a, b) in enumerate(pairs):
        entry = inner[spot : spot + 1]
        if b == ITERS:
            entry = entry + energies[a]
        gram[a, b] = gram[b, a] = entry

    def product(left, right):
        return sum(x * y * gram[a, b] for a, x in enumerate(left) for b, y in enumerate(right))

    one = jnp.ones((1, LANES), jnp.float32)
    residual, direction, solution_part = [one], [one], []
    norm = product(residual, residual)
    for step in range(ITERS):
        image = [shift_by * x for x in direction] + [jnp.zeros_like(one)]
        for a, x in enumerate(direction):
            image[a + 1] = image[a + 1] + x
        alpha = norm / product(direction, image)
        padded = solution_part + [jnp.zeros_like(one)] * (len(direction) - len(solution_part))
        solution_part = [s + alpha * x for s, x in zip(padded, direction)]
        if step + 1 < ITERS:
            longer = residual + [jnp.zeros_like(one)]
            residual = [r - alpha * i for r, i in zip(longer, image)]
            after = product(residual, residual)
            ratio = after / norm
            direction = [r + ratio * x for r, x in zip(residual, direction + [jnp.zeros_like(one)])]
            norm = after

    charges = prior[...]
    charge_part = descriptor[1].reshape(LANES, LANES)
    for a, x in enumerate(solution_part):
        charges = charges + x * vectors[a]
        charge_part = charge_part + x * descriptor[2 + a].reshape(LANES, LANES)
    charges_out[...] = charges
    inputs = jnp.concatenate([descriptor[0].reshape(LANES, LANES), charge_part], axis=0)
    inputs = (FEATURE_SCALE * inputs).astype(jnp.bfloat16)
    energies_out[...] = network(
        inputs, short_first[...], stacked(1), mid_ref[1], 4, short_offset, stacked(2) * charges
    )

    departed(halo_tile_in, tile_sems)
    for step in range(ITERS):
        departed(halo_row_in.at[step], row_sems.at[step])
    departed(dot_plane_in, dot_sems.at[0])
    departed(dot_line_in, dot_sems.at[1])
    for phase in range(ITERS + 1):
        departed(plane_in.at[phase], plane_sems.at[phase])
        departed(line_in.at[phase], line_sems.at[phase])


def body(
    sizes,
    positions,
    elements,
    prior_charges,
    neighbours,
    counts,
    boundary,
    wave_numbers,
    hardness,
    chi_first,
    chi_bias,
    chi_mid,
    chi_out,
    chi_offset,
    short_first,
    short_charge,
    short_bias,
    short_mid,
    short_out,
    short_offset,
):
    atoms = positions.shape[-1]
    halo, plane, line = plan(sizes)
    table = wave_table(sizes, atoms * sizes[0] * sizes[1] * sizes[2])
    vmem = pl.BlockSpec(memory_space=pltpu.VMEM)
    smem = pl.BlockSpec(memory_space=pltpu.SMEM)
    f32 = jnp.float32
    phases = ITERS + 1
    row = jax.ShapeDtypeStruct((1, atoms), f32)
    charges, energies = pl.pallas_call(
        functools.partial(kernel, sizes),
        out_shape=(row, row),
        in_specs=[smem] * 3 + [vmem] * 17,
        out_specs=(vmem, vmem),
        scratch_shapes=[
            pltpu.VMEM((CHUNKS, LANES, LANES), f32),
            pltpu.VMEM((CHUNKS, LANES, LANES), f32),
            pltpu.VMEM((LANES, LANES), jnp.int32),
            pltpu.VMEM((LANES, LANES), jnp.int32),
            pltpu.VMEM((LANES, LANES), f32),
            pltpu.VMEM((LANES, LANES), f32),
            pltpu.VMEM((LANES, LANES), f32),
            pltpu.VMEM((4, LANES, LANES), f32),
            pltpu.VMEM((NBASIS, LANES, LANES), f32),
            pltpu.VMEM((ITERS + 2, 4, NBASIS, LANES), f32),
            pltpu.VMEM((8, LANES), f32),
            pltpu.VMEM((8, LANES), jnp.int32),
            pltpu.VMEM((LANES, LANES), f32),
            pltpu.VMEM((2, NBASIS, LANES), f32),
            pltpu.VMEM((LANES, LANES), f32),
            pltpu.VMEM((ITERS, 16, LANES), f32),
            pltpu.VMEM((16, LANES), f32),
            pltpu.VMEM((ITERS + 1, 8, LANES), f32),
            pltpu.VMEM((8, LANES), f32),
            pltpu.VMEM((len(halo), 8, LANES), f32),
            pltpu.VMEM((ITERS, 1, LANES), f32),
            pltpu.VMEM((ITERS, len(halo), 1, LANES), f32),
            pltpu.VMEM((phases, 16, LANES), f32),
            pltpu.VMEM((phases, len(plane), 16, LANES), f32),
            pltpu.VMEM((phases, 16, LANES), f32),
            pltpu.VMEM((phases, len(line), 16, LANES), f32),
            pltpu.VMEM((16, LANES), f32),
            pltpu.VMEM((len(plane), 16, LANES), f32),
            pltpu.VMEM((16, LANES), f32),
            pltpu.VMEM((len(line), 16, LANES), f32),
            pltpu.SemaphoreType.DMA((2,)),
            pltpu.SemaphoreType.DMA((ITERS, 2)),
            pltpu.SemaphoreType.DMA((phases, 2)),
            pltpu.SemaphoreType.DMA((phases, 2)),
            pltpu.SemaphoreType.DMA((2, 2)),
        ],
        compiler_params=pltpu.CompilerParams(collective_id=0, has_side_effects=True),
    )(
        hardness,
        chi_offset,
        short_offset,
        positions.reshape(3, 1, atoms),
        elements.reshape(1, atoms),
        prior_charges.reshape(1, atoms),
        neighbours.reshape(atoms, atoms),
        counts.reshape(1, atoms),
        boundary.reshape(1, -1),
        wave_numbers,
        jnp.asarray(table),
        chi_bias,
        short_bias,
        short_charge,
        chi_out,
        short_out,
        chi_first.reshape(atoms, -1),
        chi_mid,
        short_first.reshape(atoms, -1),
        short_mid,
    )
    return (charges.reshape(1, 1, 1, atoms), energies.reshape(1, 1, 1, atoms))


def solution(mesh):
    sizes = tuple(mesh.shape[name] for name in AXES)
    spread_over = P("gx", "gy", "gz", None)
    in_specs = (
        P(None, "gx", "gy", "gz", None),
        spread_over,
        spread_over,
        P("gx", "gy", "gz", None, None),
        spread_over,
        spread_over,
    ) + (P(),) * 13
    return jax.shard_map(
        functools.partial(body, sizes),
        mesh=mesh,
        in_specs=in_specs,
        out_specs=(spread_over, spread_over),
        check_vma=False,
    )
```

```python
import functools
import math

import jax
import jax.numpy as jnp
import numpy as np
from jax import lax
from jax.experimental import pallas as pl
from jax.experimental.pallas import tpu as pltpu
from jax.sharding import PartitionSpec as P

NBASIS = 32
ITERS = 3
DOMAIN = 22.0
SOFTENING = 22.0
SCREENING = 0.005
CUTOFF = 66.0
DAMPING = 0.1
COUPLING = 64.0
FEATURE_SCALE = 0.5
PAIR_STRENGTH = 1.0
TOP = 6
LANES = 128
BINS = TOP * (2 * TOP) ** 2
CHUNKS = -(-BINS // LANES)
MESH = pl.DeviceIdType.MESH
AXES = ("gx", "gy", "gz")

OFFSETS = [
    (a, b, c) for a in (-1, 0, 1) for b in (-1, 0, 1) for c in (-1, 0, 1) if (a, b, c) != (0, 0, 0)
]


def wave_table(sizes, total_atoms):
    table = np.zeros((CHUNKS * LANES, 8), np.float64)
    signed = [n for n in range(-TOP, TOP + 1) if n != 0]
    spot = 0
    for nx in range(1, TOP + 1):
        for ny in signed:
            for nz in signed:
                k = 2.0 * np.pi * np.array([nx, ny, nz]) / (DOMAIN * np.array(sizes))
                squared = float((k * k).sum())
                weight = (
                    COUPLING * DAMPING**2 * math.exp(-squared / (4.0 * DAMPING**2)) / (squared * total_atoms)
                )
                table[spot, :4] = (nx, ny, nz, weight)
                spot += 1
    return table.reshape(CHUNKS, LANES, 8).transpose(0, 2, 1).astype(np.float32)


SIN_TERMS = [(-1) ** n * (2 * math.pi) ** (2 * n + 1) / math.factorial(2 * n + 1) for n in range(9)]
COS_TERMS = [(-1) ** n * (2 * math.pi) ** (2 * n) / math.factorial(2 * n) for n in range(10)]
ERF_TERMS = [
    2.0 / math.sqrt(math.pi) * (-1) ** n / (math.factorial(n) * (2 * n + 1)) for n in range(9)
]


def series(square, terms):
    total = jnp.full_like(square, terms[-1])
    for term in terms[-2::-1]:
        total = total * square + term
    return total


def unique_shifts(shifts, sizes):
    seen = []
    for shift in shifts:
        wrapped = tuple(s % n for s, n in zip(shift, sizes))
        if wrapped != (0, 0, 0) and wrapped not in seen:
            seen.append(wrapped)
    return seen


def negated(shift, sizes):
    return tuple((-s) % n for s, n in zip(shift, sizes))


def plan(sizes):
    halo = unique_shifts(OFFSETS, sizes)
    plane = unique_shifts([(a, b, 0) for a in range(sizes[0]) for b in range(sizes[1])], sizes)
    line = unique_shifts([(0, 0, c) for c in range(sizes[2])], sizes)
    everyone = unique_shifts(
        [(a, b, c) for a in range(sizes[0]) for b in range(sizes[1]) for c in range(sizes[2])], sizes
    )

    def nearness(shift):
        return -(2 * (shift[0] != 0) + 2 * min(shift[2], sizes[2] - shift[2]) + (shift[1] != 0))

    return tuple(sorted(shifts, key=nearness) for shifts in (halo, plane, line, everyone))


def kernel(
    sizes,
    hardness,
    chi_offset,
    short_offset,
    positions,
    elements,
    prior,
    neighbours,
    counts,
    boundary,
    waves,
    table,
    chi_bias,
    short_bias,
    short_charge,
    chi_out,
    short_out,
    chi_first,
    chi_mid,
    short_first,
    short_mid,
    charges_out,
    energies_out,
    tile_cos,
    tile_sin,
    low_ref,
    high_ref,
    pair_ref,
    reach_ref,
    taper_ref,
    weights_ref,
    basis_ref,
    descriptor,
    own_ref,
    picks_ref,
    pack_ref,
    mid_ref,
    near_kind_ref,
    totals_ref,
    wave_weights,
    extended,
    halo_tile_out,
    halo_tile_in,
    halo_row_out,
    halo_row_in,
    plane_out,
    plane_in,
    line_out,
    line_in,
    dots,
    dots_out,
    dots_in,
    tile_sems,
    row_sems,
    plane_sems,
    line_sems,
    dot_sems,
):
    halo, plane, line, everyone = plan(sizes)
    place = [lax.axis_index(name) for name in AXES]

    def device(shift):
        return tuple(lax.rem(p + s, n) if s else p for p, s, n in zip(place, shift, sizes))

    barrier = pltpu.get_barrier_semaphore()
    for shift in everyone:
        pl.semaphore_signal(barrier, inc=1, device_id=device(shift), device_id_type=MESH)

    square = (LANES, LANES)

    def send(shifts, source, landing, sems):
        for shift in shifts:
            pltpu.make_async_remote_copy(
                src_ref=source,
                dst_ref=landing.at[shifts.index(negated(shift, sizes))],
                send_sem=sems.at[0],
                recv_sem=sems.at[1],
                device_id=device(shift),
                device_id_type=MESH,
            ).start()

    def landed(landing, sems):
        pltpu.make_async_copy(landing, landing, sems.at[1]).wait()

    def departed(landing, sems):
        pltpu.make_async_copy(landing, landing, sems.at[0]).wait()

    def column(row):
        return jnp.broadcast_to(row, square).T

    def pick_lanes(source, index):
        return jnp.take_along_axis(source, index, axis=1, mode="promise_in_bounds")

    own_ref[...] = jnp.zeros((8, LANES), jnp.float32)
    for d in range(3):
        own_ref[d : d + 1, :] = positions[d]
    own_ref[3:4, :] = elements[...].astype(jnp.float32)
    own_ref[4:5, :] = prior[...]
    lane8 = lax.broadcasted_iota(jnp.int32, (8, LANES), 1)
    width = boundary.shape[1]
    picks_ref[...] = jnp.zeros((8, LANES), jnp.int32)
    picks_ref[0:1, 0:width] = boundary[...]
    picks8 = pick_lanes(jnp.broadcast_to(picks_ref[0:1, :], (8, LANES)), lane8 & (width - 1))
    halo_tile_out[...] = pick_lanes(own_ref[...], picks8)

    def structure(row, target):
        values = column(row)
        target[...] = jnp.zeros((16, LANES), jnp.float32)
        for c in range(CHUNKS):
            target[c : c + 1, :] = jnp.sum(tile_cos[c] * values, axis=0, keepdims=True)
            target[8 + c : 9 + c, :] = jnp.sum(tile_sin[c] * values, axis=0, keepdims=True)

    def spread(weighted):
        total = jnp.zeros(square, jnp.float32)
        for c in range(CHUNKS):
            total = total + tile_cos[c] * weighted[c : c + 1] + tile_sin[c] * weighted[8 + c : 9 + c]
        return jnp.sum(total.T, axis=0, keepdims=True)

    def reduce_start(phase):
        send(plane, plane_out.at[phase], plane_in.at[phase], plane_sems.at[phase])

    def reduce_middle(phase):
        landed(plane_in.at[phase], plane_sems.at[phase])
        line_out[phase] = plane_out[phase] + jnp.sum(plane_in[phase], axis=0)
        send(line, line_out.at[phase], line_in.at[phase], line_sems.at[phase])

    def reduce_end(phase):
        landed(line_in.at[phase], line_sems.at[phase])
        return line_out[phase] + jnp.sum(line_in[phase], axis=0)

    pl.semaphore_wait(barrier, len(everyone))
    send(halo, halo_tile_out, halo_tile_in, tile_sems)

    turns = [
        column(
            (positions[d] + DOMAIN * place[d].astype(jnp.float32)) * (1.0 / (DOMAIN * sizes[d]))
        )
        for d in range(3)
    ]

    def fill(c, carry):
        lanes = table[c]
        theta = turns[0] * lanes[0:1] + turns[1] * lanes[1:2] + turns[2] * lanes[2:3]
        theta = theta - jnp.round(theta)
        squared = theta * theta
        tile_cos[c] = series(squared, COS_TERMS)
        tile_sin[c] = theta * series(squared, SIN_TERMS)
        return carry

    lax.fori_loop(0, CHUNKS, fill, 0)

    structure(prior[...], plane_out.at[0])
    reduce_start(0)

    nearby = neighbours[...].T
    low_ref[...] = nearby & (LANES - 1)
    high_ref[...] = nearby >> 7
    lane_row = lax.broadcasted_iota(jnp.int32, (1, LANES), 1)
    row8 = lax.broadcasted_iota(jnp.int32, (8, LANES), 0)
    deep = lax.broadcasted_iota(jnp.int32, square, 0)

    def tally(p, sums):
        at = pl.ds(pl.multiple_of(p * LANES, LANES), LANES)
        nx, ny, nz = (waves[d : d + 1, at] for d in range(3))
        flip = jnp.where(nx < 0, -1, 1)
        nx, ny, nz = nx * flip, ny * flip, nz * flip
        ny = ny + jnp.where(ny < 0, TOP, TOP - 1)
        nz = nz + jnp.where(nz < 0, TOP, TOP - 1)
        spots = column((((nx - 1) * (2 * TOP) + ny) * (2 * TOP) + nz).astype(jnp.float32))
        return tuple(
            total
            + jnp.sum(
                jnp.where(spots == (lane_row + c * LANES).astype(jnp.float32), 1.0, 0.0), axis=0, keepdims=True
            )
            for c, total in enumerate(sums)
        )

    zero_row = jnp.zeros((1, LANES), jnp.float32)
    many = lax.fori_loop(0, waves.shape[1] // LANES, tally, (zero_row,) * CHUNKS)
    wave_weights[...] = jnp.zeros((16, LANES), jnp.float32)
    for c in range(CHUNKS):
        weighted_row = many[c] * table[c, 3:4, :]
        wave_weights[c : c + 1, :] = weighted_row
        wave_weights[8 + c : 9 + c, :] = weighted_row

    kind_row = elements[...]
    kinds = [jnp.where(kind_row == e, 1.0, 0.0) for e in range(4)]
    kind_mask = jnp.where((deep >> 5) == kind_row, 1.0, 0.0)
    stiffness = sum(kinds[e] * hardness[e] for e in range(4))
    shift_by = 0.25 * (hardness[0] + hardness[1] + hardness[2] + hardness[3])

    pack_ref[...] = jnp.zeros(square, jnp.float32)
    for spot, part in enumerate((chi_bias, short_bias, short_charge, chi_out, short_out)):
        pack_ref[4 * spot : 4 * spot + 4, 0:32] = part[...]
    pack_ref[...] = pack_ref[...].T

    def parameter(spot):
        return [pack_ref[0:32, 4 * spot + e : 4 * spot + e + 1] for e in range(4)]

    def stacked(spot):
        return jnp.concatenate([jnp.broadcast_to(x, (32, LANES)) for x in parameter(spot)], axis=0)

    for spot, mid in enumerate((chi_mid, short_mid)):
        wide = mid[...].astype(jnp.float32)
        for e in range(4):
            mid_ref[spot, :, 32 * e : 32 * e + 32] = wide[:, e, :]

    reduce_middle(0)
    landed(halo_tile_in, tile_sems)

    slots = [halo.index(tuple(s % n for s, n in zip(o, sizes))) for o in OFFSETS]

    def merge(fetch, lanes, chunk):
        out = fetch(4 * chunk)
        for q in range(1, 4):
            if 4 * chunk + q < len(OFFSETS):
                out = jnp.where(lanes >= 32 * q, fetch(4 * chunk + q), out)
        return out

    def moved(block):
        o = OFFSETS[block]
        by = jnp.where(
            row8 == 0, DOMAIN * o[0], jnp.where(row8 == 1, DOMAIN * o[1], jnp.where(row8 == 2, DOMAIN * o[2], 0.0))
        )
        return halo_tile_in[slots[block]] + by

    tiles = [own_ref[...]] + [merge(moved, lane8, c) for c in range(7)]

    def gather(rows):
        low, high = low_ref[...], high_ref[...]
        out = jnp.zeros(square, jnp.float32)
        for c in range(8):
            out = jnp.where(high == c, pick_lanes(jnp.broadcast_to(rows[c], square), low), out)
        return out

    total = jnp.zeros(square, jnp.float32)
    for d in range(3):
        gap = gather([tile[d : d + 1] for tile in tiles]) - positions[d]
        total = total + gap * gap
    distance = jnp.sqrt(total)
    valid = jnp.where(deep < counts[...], 1.0, 0.0)
    soft_square = total + SOFTENING * SOFTENING
    soft = jnp.sqrt(soft_square)
    far = SCREENING * soft
    erfc = 1.0 - far * series(far * far, ERF_TERMS)
    pair_ref[...] = valid * (PAIR_STRENGTH / LANES * SOFTENING) * erfc / soft
    half = jnp.minimum(distance, CUTOFF) * (0.5 / CUTOFF)
    taper_ref[...] = valid * 0.5 * (1.0 + series(half * half, COS_TERMS))
    reach_ref[...] = distance * ((NBASIS - 1) / CUTOFF)
    near_kind = gather([tile[3:4] for tile in tiles])
    near_kind_ref[...] = near_kind
    for e in range(4):
        weights_ref[e] = jnp.where(near_kind == float(e), 1.0, 0.0)
    for c in range(8):
        extended[0, c : c + 1, :] = tiles[c][4:5]

    def describe(m, carry):
        away = reach_ref[...] - m.astype(jnp.float32)
        basis = jnp.exp(-0.5 * (away * away)) * taper_ref[...]
        basis_ref[m] = basis
        for e in range(4):
            descriptor[0, e, pl.ds(m, 1), :] = jnp.sum(basis * weights_ref[e], axis=0, keepdims=True)
        return carry

    lax.fori_loop(0, NBASIS, describe, 0)

    def network(inputs, first_weights, bias, mid, out_spot, offset):
        activation = jnp.dot(first_weights, inputs, preferred_element_type=jnp.float32) + bias
        first = (jnp.tanh(activation) * kind_mask).astype(jnp.bfloat16)
        second = jnp.tanh(jnp.dot(mid.astype(jnp.bfloat16), first, preferred_element_type=jnp.float32))
        chosen = sum(x * kinds[e] for e, x in enumerate(parameter(out_spot)))
        result = jnp.sum(second * chosen, axis=0, keepdims=True)
        return result + sum(kinds[e] * offset[e] for e in range(4))

    features = (FEATURE_SCALE * descriptor[0].reshape(LANES, LANES)).astype(jnp.bfloat16)
    negativity = network(features, chi_first[...], stacked(0), mid_ref[0], 3, chi_offset)
    short_bias_part = stacked(1) + jnp.dot(
        short_first[:, 0:LANES], features, preferred_element_type=jnp.float32
    )

    def local(vector, phase):
        near = gather([extended[phase, c : c + 1, :] for c in range(8)])
        return near, stiffness * vector + jnp.sum(pair_ref[...] * near, axis=0, keepdims=True)

    def describe_charges(near, phase):
        for e in range(4):
            weights_ref[e] = jnp.where(near_kind_ref[...] == float(e), near, 0.0)

        def part(m, carry):
            basis = basis_ref[m]
            for e in range(4):
                descriptor[1 + phase, e, pl.ds(m, 1), :] = jnp.sum(
                    basis * weights_ref[e], axis=0, keepdims=True
                )
            return carry

        lax.fori_loop(0, NBASIS, part, 0)

    near, near_part = local(prior[...], 0)
    vector = -negativity - (near_part + spread(wave_weights[...] * reduce_end(0)))
    vectors = [vector]
    for step in range(ITERS):
        phase = step + 1
        picked = pick_lanes(jnp.broadcast_to(vector, (8, LANES)), picks8)
        halo_row_out[step] = picked[0:1]
        if phase == ITERS:
            send(halo, halo_row_out.at[step], halo_row_in.at[step], row_sems.at[step])
        structure(vector, plane_out.at[phase])
        reduce_start(phase)
        if phase < ITERS:
            send(halo, halo_row_out.at[step], halo_row_in.at[step], row_sems.at[step])
        describe_charges(near, step)
        reduce_middle(phase)
        landed(halo_row_in.at[step], row_sems.at[step])
        extended[phase, 0:1, :] = vector
        for c in range(7):
            extended[phase, c + 1 : c + 2, :] = merge(lambda b: halo_row_in[step, slots[b]], lane_row, c)
        near, near_part = local(vector, phase)
        near_part = near_part - shift_by * vector
        if phase < ITERS:
            totals_ref[step] = reduce_end(phase)
            vector = near_part + spread(wave_weights[...] * totals_ref[step])
            vectors.append(vector)

    pairs = [(a, b) for a in range(ITERS) for b in range(a, ITERS)]
    rows = [vectors[a] * vectors[b] for a, b in pairs] + [x * near_part for x in vectors]
    pairs = pairs + [(a, ITERS) for a in range(ITERS)]
    dots[...] = jnp.zeros((16, LANES), jnp.float32)
    for spot, row in enumerate(rows):
        dots[spot : spot + 1, :] = row
    diagonal = lax.broadcasted_iota(jnp.int32, (16, LANES), 0) == lax.broadcasted_iota(
        jnp.int32, (16, LANES), 1
    )
    dots_out[...] = jnp.sum(
        jnp.where(diagonal, jnp.sum(dots[...], axis=1, keepdims=True), 0.0), axis=0, keepdims=True
    )
    send(everyone, dots_out, dots_in, dot_sems)
    describe_charges(near, ITERS)
    totals_ref[ITERS - 1] = reduce_end(ITERS)
    weighted = wave_weights[...] * totals_ref[ITERS - 1]
    energies = [
        jnp.sum(jnp.sum(weighted * totals_ref[a], axis=0, keepdims=True), axis=1, keepdims=True)
        for a in range(ITERS)
    ]
    landed(dots_in, dot_sems)
    inner = jnp.broadcast_to(dots_out[...] + jnp.sum(dots_in[...], axis=0), (16, LANES))
    inner = jnp.sum(jnp.where(diagonal, inner, 0.0), axis=1, keepdims=True)
    inner = jnp.broadcast_to(inner, (16, LANES))
    gram = {}
    for spot, (a, b) in enumerate(pairs):
        entry = inner[spot : spot + 1]
        if b == ITERS:
            entry = entry + energies[a]
        gram[a, b] = gram[b, a] = entry

    def product(left, right):
        return sum(x * y * gram[a, b] for a, x in enumerate(left) for b, y in enumerate(right))

    one = jnp.ones((1, LANES), jnp.float32)
    residual, direction, solution_part = [one], [one], []
    norm = product(residual, residual)
    for step in range(ITERS):
        image = [shift_by * x for x in direction] + [jnp.zeros_like(one)]
        for a, x in enumerate(direction):
            image[a + 1] = image[a + 1] + x
        alpha = norm / product(direction, image)
        padded = solution_part + [jnp.zeros_like(one)] * (len(direction) - len(solution_part))
        solution_part = [s + alpha * x for s, x in zip(padded, direction)]
        if step + 1 < ITERS:
            longer = residual + [jnp.zeros_like(one)]
            residual = [r - alpha * i for r, i in zip(longer, image)]
            after = product(residual, residual)
            ratio = after / norm
            direction = [r + ratio * x for r, x in zip(residual, direction + [jnp.zeros_like(one)])]
            norm = after

    charges = prior[...]
    charge_part = descriptor[1].reshape(LANES, LANES)
    for a, x in enumerate(solution_part):
        charges = charges + x * vectors[a]
        charge_part = charge_part + x * descriptor[2 + a].reshape(LANES, LANES)
    charges_out[...] = charges
    inputs = (FEATURE_SCALE * charge_part).astype(jnp.bfloat16)
    energies_out[...] = network(
        inputs,
        short_first[:, LANES : 2 * LANES],
        short_bias_part + stacked(2) * charges,
        mid_ref[1],
        4,
        short_offset,
    )

    departed(halo_tile_in, tile_sems)
    for step in range(ITERS):
        departed(halo_row_in.at[step], row_sems.at[step])
    departed(dots_in, dot_sems)
    for phase in range(ITERS + 1):
        departed(plane_in.at[phase], plane_sems.at[phase])
        departed(line_in.at[phase], line_sems.at[phase])


def body(
    sizes,
    positions,
    elements,
    prior_charges,
    neighbours,
    counts,
    boundary,
    wave_numbers,
    hardness,
    chi_first,
    chi_bias,
    chi_mid,
    chi_out,
    chi_offset,
    short_first,
    short_charge,
    short_bias,
    short_mid,
    short_out,
    short_offset,
):
    atoms = positions.shape[-1]
    halo, plane, line, everyone = plan(sizes)
    table = wave_table(sizes, atoms * sizes[0] * sizes[1] * sizes[2])
    vmem = pl.BlockSpec(memory_space=pltpu.VMEM)
    smem = pl.BlockSpec(memory_space=pltpu.SMEM)
    f32 = jnp.float32
    phases = ITERS + 1
    row = jax.ShapeDtypeStruct((1, atoms), f32)
    charges, energies = pl.pallas_call(
        functools.partial(kernel, sizes),
        out_shape=(row, row),
        in_specs=[smem] * 3 + [vmem] * 17,
        out_specs=(vmem, vmem),
        scratch_shapes=[
            pltpu.VMEM((CHUNKS, LANES, LANES), f32),
            pltpu.VMEM((CHUNKS, LANES, LANES), f32),
            pltpu.VMEM((LANES, LANES), jnp.int32),
            pltpu.VMEM((LANES, LANES), jnp.int32),
            pltpu.VMEM((LANES, LANES), f32),
            pltpu.VMEM((LANES, LANES), f32),
            pltpu.VMEM((LANES, LANES), f32),
            pltpu.VMEM((4, LANES, LANES), f32),
            pltpu.VMEM((NBASIS, LANES, LANES), f32),
            pltpu.VMEM((ITERS + 2, 4, NBASIS, LANES), f32),
            pltpu.VMEM((8, LANES), f32),
            pltpu.VMEM((8, LANES), jnp.int32),
            pltpu.VMEM((LANES, LANES), f32),
            pltpu.VMEM((2, NBASIS, LANES), f32),
            pltpu.VMEM((LANES, LANES), f32),
            pltpu.VMEM((ITERS, 16, LANES), f32),
            pltpu.VMEM((16, LANES), f32),
            pltpu.VMEM((ITERS + 1, 8, LANES), f32),
            pltpu.VMEM((8, LANES), f32),
            pltpu.VMEM((len(halo), 8, LANES), f32),
            pltpu.VMEM((ITERS, 1, LANES), f32),
            pltpu.VMEM((ITERS, len(halo), 1, LANES), f32),
            pltpu.VMEM((phases, 16, LANES), f32),
            pltpu.VMEM((phases, len(plane), 16, LANES), f32),
            pltpu.VMEM((phases, 16, LANES), f32),
            pltpu.VMEM((phases, len(line), 16, LANES), f32),
            pltpu.VMEM((16, LANES), f32),
            pltpu.VMEM((1, LANES), f32),
            pltpu.VMEM((len(everyone), 1, LANES), f32),
            pltpu.SemaphoreType.DMA((2,)),
            pltpu.SemaphoreType.DMA((ITERS, 2)),
            pltpu.SemaphoreType.DMA((phases, 2)),
            pltpu.SemaphoreType.DMA((phases, 2)),
            pltpu.SemaphoreType.DMA((2,)),
        ],
        compiler_params=pltpu.CompilerParams(collective_id=0, has_side_effects=True),
    )(
        hardness,
        chi_offset,
        short_offset,
        positions.reshape(3, 1, atoms),
        elements.reshape(1, atoms),
        prior_charges.reshape(1, atoms),
        neighbours.reshape(atoms, atoms),
        counts.reshape(1, atoms),
        boundary.reshape(1, -1),
        wave_numbers,
        jnp.asarray(table),
        chi_bias,
        short_bias,
        short_charge,
        chi_out,
        short_out,
        chi_first.reshape(atoms, -1),
        chi_mid,
        short_first.reshape(atoms, -1),
        short_mid,
    )
    return (charges.reshape(1, 1, 1, atoms), energies.reshape(1, 1, 1, atoms))


def solution(mesh):
    sizes = tuple(mesh.shape[name] for name in AXES)
    spread_over = P("gx", "gy", "gz", None)
    in_specs = (
        P(None, "gx", "gy", "gz", None),
        spread_over,
        spread_over,
        P("gx", "gy", "gz", None, None),
        spread_over,
        spread_over,
    ) + (P(),) * 13
    return jax.shard_map(
        functools.partial(body, sizes),
        mesh=mesh,
        in_specs=in_specs,
        out_specs=(spread_over, spread_over),
        check_vma=False,
    )
```
